32 devices in a mesh: rep: 1, fsdp: 32 (over z, y, x, core).
Axes of the slice: x: 2, y: 2, z: 4, core: 2. Of those that a mesh axis runs over, the one named last changes fastest.
Arguments:
- grads: bfloat16 [1, 24, 1280, 1280], P('rep', None, 'fsdp'), as said below
- group_counts: int32 [2], replicated, may hold values from 1 to 18, 24 in all
- owners: int32 [24], replicated, may hold values from 0 to 31, as said below
- left_stat: float32 [32, 1280, 1280], P('fsdp', 'rep'), may hold values from -4 to 4
- right_stat: float32 [32, 1280, 1280], P('fsdp', 'rep'), may hold values from -4 to 4
- left_root: bfloat16 [32, 1280, 1280], P('fsdp', 'rep'), as said below
- right_root: bfloat16 [32, 1280, 1280], P('fsdp', 'rep'), as said below
Outputs:
- left_new: float32 [32, 1280, 1280], P('fsdp', 'rep')
- right_new: float32 [32, 1280, 1280], P('fsdp', 'rep')
- update: bfloat16 [24, 1280, 1280], P(None, ('rep', 'fsdp'))
The draws below stay inside these ranges and needn't reach their ends.
Inputs may be any that keep to these rules, and one draw needn't show every extreme that they name: `grads`: block gradients of every replica group, real-valued. `owners`: no slot is named by two blocks. `group_counts`: the counts add up to 24. `left_root`: Symmetric, with a positive diagonal of about 0.5 to 2, each entry within a small symmetric perturbation of that range, and off-diagonal entries much smaller than the diagonal. `right_root`: Symmetric, with a positive diagonal of about 0.5 to 2, each entry within a small symmetric perturbation of that range, and off-diagonal entries much smaller than the diagonal.
All inputs are finite; a program needn't handle non-finite values.
Results may differ from the reference program's by a relative error of at most 0.00065.
The reference program's roundings to bfloat16 on the way count: a program that leaves them out, or rounds other values in their place, can miss the bound.
Values may be sent and summed in bfloat16 or wider, within the bound.
A program may use at most 128 MiB of HBM per device.

```python
import math
import jax
import jax.numpy as jnp
import numpy as np
from jax import lax

W = 1280
REPS = 1
SLOTS = 32
NB = 24
GROUPS = 2
GROUP_MOST = 18


def draw_grads(key, part):
    keys = jax.random.split(key, 4)
    block_scale = jnp.exp(jax.random.uniform(keys[0], (1, NB, 1, 1), jnp.float32, math.log(0.5), math.log(2.0)))
    row_scale = jnp.exp(jax.random.uniform(keys[1], (1, 1, W, 1), jnp.float32, math.log(0.3), math.log(3.0)))
    column_scale = jnp.exp(jax.random.uniform(keys[2], (1, 1, 1, W), jnp.float32, math.log(0.3), math.log(3.0)))
    base = jax.random.normal(keys[3], (REPS, NB, W, W), jnp.float32)
    return (base * block_scale * row_scale * column_scale).astype(jnp.bfloat16)


def draw_owners(key, part):
    return jax.random.permutation(key, SLOTS)[:NB].astype(jnp.int32)


def root_matrix(key):
    keys = jax.random.split(key, 2)
    noise = jax.random.normal(keys[0], (SLOTS, W, W), jnp.float32)
    noise = noise * (0.5 / math.sqrt(W))
    symmetric = (noise + jnp.swapaxes(noise, 1, 2)) / math.sqrt(2.0)
    diagonal = jnp.exp(jax.random.uniform(keys[1], (SLOTS, W), jnp.float32, math.log(0.5), math.log(2.0)))
    return symmetric + diagonal[:, :, None] * jnp.eye(W, dtype=jnp.float32)[None, :, :]


def draw_left_root(key, part):
    return root_matrix(jax.random.fold_in(key, 11)).astype(jnp.bfloat16)


def draw_right_root(key, part):
    return root_matrix(jax.random.fold_in(key, 23)).astype(jnp.bfloat16)


def level_of(rng, extent, pieces, smallest, high):
    gain, own = 1.0, jax.random.fold_in(rng, 6)
    for dim, parts in pieces:
        steps = jnp.exp(jax.random.uniform(jax.random.fold_in(own, dim), (parts,), jnp.float32, smallest / len(pieces), high / len(pieces)))
        gain = gain * jnp.repeat(steps, extent[dim] // parts).reshape([-1 if axis == dim else 1 for axis in range(len(extent))])
    return gain


def split_up(count, total, reach, slope):
    weights = [(1 << 20) // math.isqrt(grade ** slope) + 1 for grade in range(2, count + 1)]
    surplus, counts = total - reach - (count - 1), [1] * (count - 1)
    while surplus > 0:
        candidates = [i for i in range(count - 1) if counts[i] < reach]
        whole, left = sum([weights[i] for i in candidates]), surplus
        for i in candidates:
            addition = min(reach - counts[i], max(1, left * weights[i] // whole), surplus)
            counts[i] = counts[i] + addition
            surplus = surplus - addition
    return np.array([reach] + counts)


def ragged_sizes(own_key, count, total, reach, skew):
    if count == 2:
        one = jax.random.randint(own_key, (), max(1, total - reach), min(reach, total - 1) + 1)
        return jnp.stack([one, total - one])
    lengths = jnp.asarray(split_up(count, total, reach, skew), jnp.int32)
    pairs = (count - 1) // 2
    donor, sink = lengths[1:1 + 2 * pairs:2], lengths[2:2 + 2 * pairs:2]
    margin = jnp.minimum(donor - 1, reach - sink)
    moved = jax.random.randint(jax.random.fold_in(own_key, 1), (pairs,), 0, 1 << 20) % (margin + 1)
    lengths = lengths.at[1:1 + 2 * pairs:2].set(donor - moved).at[2:2 + 2 * pairs:2].set(sink + moved)
    return lengths[jax.random.permutation(jax.random.fold_in(own_key, 2), count)]


def normal_values(key, extent, deviation, reach, cuts=(), kind=jnp.bfloat16):
    drawn = deviation * jax.random.normal(key, extent, jnp.float32)
    if cuts:
        drawn = drawn * level_of(key, extent, cuts, -0.22, 0.18)
    return jnp.clip(drawn, -reach, reach).astype(kind)


def setup_inputs(seed: int = 0) -> dict:
    seeds = jax.random.split(jax.random.key(seed), 8)
    grads = draw_grads(jax.random.fold_in(seeds[7], 71), 0)
    group_counts = ragged_sizes(seeds[1], GROUPS, NB, GROUP_MOST, 1).astype(jnp.int32)
    owners = draw_owners(jax.random.fold_in(seeds[7], 71), 0)
    left_stat = normal_values(seeds[3], (SLOTS, W, W), 0.5, 4.0, ((0, 32),), jnp.float32)
    right_stat = normal_values(seeds[4], (SLOTS, W, W), 0.5, 4.0, ((0, 32),), jnp.float32)
    left_root = draw_left_root(jax.random.fold_in(seeds[7], 71), 0)
    right_root = draw_right_root(jax.random.fold_in(seeds[7], 71), 0)
    return dict(grads=grads, group_counts=group_counts, owners=owners, left_stat=left_stat, right_stat=right_stat, left_root=left_root, right_root=right_root)


BETA = 0.95
EPSILON = 1e-06

def one_block(items):
    block, left_one, right_one = items
    left_gram = jnp.dot(block, block.T, preferred_element_type=jnp.float32)
    right_gram = jnp.dot(block.T, block, preferred_element_type=jnp.float32)
    halfway = jnp.dot(left_one, block, preferred_element_type=jnp.float32).astype(jnp.bfloat16)
    precond = jnp.dot(halfway, right_one, preferred_element_type=jnp.float32)
    return (left_gram, right_gram, precond)

def reference(grads, group_counts, owners, left_stat, right_stat, left_root, right_root):
    grad = lax.optimization_barrier(jnp.sum(grads.astype(jnp.float32), axis=0)).astype(jnp.bfloat16)
    width = grad.shape[1]
    coef = (1.0 - BETA) / width
    left_gram, right_gram, precond = lax.map(one_block, (grad, left_root[owners], right_root[owners]))
    left_new = BETA * left_stat + coef * jnp.zeros_like(left_stat).at[owners].set(left_gram)
    right_new = BETA * right_stat + coef * jnp.zeros_like(right_stat).at[owners].set(right_gram)
    ends = jnp.cumsum(group_counts).astype(jnp.int32)
    starts = (ends - group_counts).astype(jnp.int32)
    block_ids = jnp.arange(grad.shape[0], dtype=jnp.int32)
    member = ((block_ids[:, None] >= starts[None, :]) & (block_ids[:, None] < ends[None, :])).astype(jnp.float32)
    grad_f = grad.astype(jnp.float32)
    block_gsq = lax.optimization_barrier(jnp.sum(grad_f * grad_f, axis=(1, 2)))
    block_psq = lax.optimization_barrier(jnp.sum(precond * precond, axis=(1, 2)))
    grad_sq = lax.optimization_barrier(jnp.sum(member * block_gsq[:, None], axis=0))
    prec_sq = lax.optimization_barrier(jnp.sum(member * block_psq[:, None], axis=0))
    group_ratio = jnp.sqrt((grad_sq + EPSILON) / (prec_sq + EPSILON))
    block_ratio = lax.optimization_barrier(jnp.sum(member * group_ratio[None, :], axis=1))
    update = (precond * block_ratio[:, None, None]).astype(jnp.bfloat16)
    return (left_new, right_new, update)
```

```python
import jax
import jax.numpy as jnp
from jax import lax
from jax.sharding import PartitionSpec as P

BETA = 0.95
EPSILON = 1e-06


def on_device(grads, group_counts, owners, left_stat, right_stat, left_root, right_root):
    slots = lax.axis_size("fsdp")
    width = left_stat.shape[2]
    half_rows = left_stat.shape[1]
    slot_ids = jnp.arange(slots, dtype=jnp.int32)
    placing = (owners[:, None] == slot_ids[None, :]).astype(jnp.bfloat16)
    local = grads[0]
    summed = lax.psum(local, "rep").astype(jnp.float32).astype(jnp.bfloat16)
    slotted = jnp.einsum("bs,brc->src", placing, summed, preferred_element_type=jnp.float32).astype(
        jnp.bfloat16
    )
    rows = local.shape[1]
    block = lax.all_to_all(slotted, "fsdp", split_axis=0, concat_axis=0, tiled=True)
    block = block.reshape(slots * rows, width)
    first = lax.axis_index("rep") * half_rows
    mine = lax.dynamic_slice_in_dim(block, first, half_rows, 0)
    columns = lax.dynamic_slice_in_dim(block, first, half_rows, 1)
    coef = (1.0 - BETA) / width
    left_gram = jnp.dot(mine, block.T, preferred_element_type=jnp.float32)
    right_gram = lax.dot_general(
        columns, block, (((0,), (0,)), ((), ())), preferred_element_type=jnp.float32
    )
    left_new = BETA * left_stat[0] + coef * left_gram
    right_new = BETA * right_stat[0] + coef * right_gram
    whole_root = lax.all_gather(right_root, "rep", axis=1, tiled=True)[0]
    halfway = jnp.dot(left_root[0], block, preferred_element_type=jnp.float32).astype(jnp.bfloat16)
    precond = jnp.dot(halfway, whole_root, preferred_element_type=jnp.float32)
    ends = jnp.cumsum(group_counts)
    starts = ends - group_counts
    block_ids = jnp.arange(owners.shape[0], dtype=jnp.int32)
    member = (
        (block_ids[:, None] >= starts[None, :]) & (block_ids[:, None] < ends[None, :])
    ).astype(jnp.float32)
    owned_here = (owners == lax.axis_index("fsdp")).astype(jnp.float32)
    my_groups = jnp.sum(owned_here[:, None] * member, axis=0)
    mine_float = mine.astype(jnp.float32)
    grad_part = my_groups * jnp.sum(mine_float * mine_float)
    prec_part = my_groups * jnp.sum(precond * precond)
    grad_sq, prec_sq = lax.psum((grad_part, prec_part), ("rep", "fsdp"))
    ratio = jnp.sum(my_groups * jnp.sqrt((grad_sq + EPSILON) / (prec_sq + EPSILON)))
    scaled = (precond * ratio).astype(jnp.bfloat16)
    pieces = scaled.reshape(slots, half_rows // slots, width)
    returned = lax.all_to_all(pieces, "fsdp", split_axis=0, concat_axis=0, tiled=True)
    update = jnp.einsum(
        "bs,srw->brw", placing, returned, preferred_element_type=jnp.float32
    ).astype(jnp.bfloat16)
    return (left_new[None], right_new[None], update)


def solution(mesh):
    in_specs = (
        P("rep", None, "fsdp", None),
        P(),
        P(),
        P("fsdp", "rep", None),
        P("fsdp", "rep", None),
        P("fsdp", "rep", None),
        P("fsdp", "rep", None),
    )
    out_specs = (P("fsdp", "rep", None), P("fsdp", "rep", None), P(None, ("rep", "fsdp"), None))
    return jax.shard_map(
        on_device, mesh=mesh, in_specs=in_specs, out_specs=out_specs, check_vma=False
    )
```
